32 devices in a mesh: rep: 2 (over z, core), dp: 16 (over x, y).
Axes of the slice: x: 4, y: 4, z: 1, core: 2. Of those that a mesh axis runs over, the one named last changes fastest.
The devices are a block of a 4x4x8 slice.
Arguments:
- x: bfloat16 [32, 2048, 640], P(('rep', 'dp')), parts along dimension 0
- dy: bfloat16 [32, 2048, 640], P(('rep', 'dp')), parts along dimension 0
- wq: bfloat16 [2, 640, 1536], P(None, 'dp')
- wk: bfloat16 [2, 640, 128], P(None, 'dp')
- wv: bfloat16 [2, 640, 128], P(None, 'dp')
- wo: bfloat16 [2, 1536, 640], P(None, 'dp')
- w_gate: bfloat16 [2, 640, 1536], P(None, 'dp')
- w_up: bfloat16 [2, 640, 1536], P(None, 'dp')
- w_down: bfloat16 [2, 1536, 640], P(None, 'dp')
Outputs:
- output 1: bfloat16 [32, 2048, 640], P(('rep', 'dp')), parts along dimension 0
- output 2: bfloat16 [4, 640, 1536], P('rep', 'dp'), parts along dimension 0
- output 3: bfloat16 [4, 640, 128], P('rep', 'dp'), parts along dimension 0
- output 4: bfloat16 [4, 640, 128], P('rep', 'dp'), parts along dimension 0
- output 5: bfloat16 [4, 1536, 640], P('rep', 'dp'), parts along dimension 0
- output 6: bfloat16 [4, 640, 1536], P('rep', 'dp'), parts along dimension 0
- output 7: bfloat16 [4, 640, 1536], P('rep', 'dp'), parts along dimension 0
- output 8: bfloat16 [4, 1536, 640], P('rep', 'dp'), parts along dimension 0
There are 2 independent parts. The reference program is written for one: setup_inputs(seed, part) draws one part's arguments, and reference() takes and returns one part's arrays. A program takes and returns all parts, laid end to end along the dimension named above; an argument that names none is the same for every part.
All inputs are finite; a program needn't handle non-finite values.
Results may differ from the reference program's by a relative error of at most 0.0255.
Values are sent between devices in bfloat16 or wider.
A program may use at most 768 MiB of HBM per device.

```python
import jax
import jax.numpy as jnp
from jax import lax

SEQUENCES = 16
TOKENS = 2048
D = 640
HEADS = 12
KV_HEADS = 1
HEAD = 128
FF = 1536
LAYERS = 2
THETA = 10000
NAMES = ("wq", "wk", "wv", "wo", "w_gate", "w_up", "w_down")
SHAPES = {
    "wq": (LAYERS, D, HEADS * HEAD),
    "wk": (LAYERS, D, KV_HEADS * HEAD),
    "wv": (LAYERS, D, KV_HEADS * HEAD),
    "wo": (LAYERS, HEADS * HEAD, D),
    "w_gate": (LAYERS, D, FF),
    "w_up": (LAYERS, D, FF),
    "w_down": (LAYERS, FF, D),
}


def bump(key, n, height):
    away = (jnp.arange(n, dtype=jnp.int32) - jax.random.randint(key, (), 0, n, jnp.int32)) % n
    return jnp.where(away < n // 8, height, 1.0)


def together(key, own, strength):
    shared = jax.random.normal(key, own.shape[1:], jnp.float32)
    return (own + strength * shared) * lax.rsqrt(1 + strength * strength)


def setup_inputs(seed: int = 0, part: int = 0) -> dict:
    kx, kdy, ka, kb, kz, kf, kh, kl, *keys = jax.random.split(jax.random.key(seed), 8 + 3 * len(NAMES))
    kx, kdy, ka, kb = (jax.random.fold_in(k, part) for k in (kx, kdy, ka, kb))
    kw, km, kv = (keys[i::3] for i in range(3))
    shape = (SEQUENCES, TOKENS, D)
    much_x, much_dy = jax.random.uniform(kz, (2,), jnp.float32, 0.0, 1.0)
    loud = 2.0 ** jax.random.uniform(jax.random.fold_in(kz, 1), (), jnp.float32, -1.0, 2.0)
    layers = 2.0 ** jax.random.uniform(kl, (LAYERS, 1, 1), jnp.float32, -1.0, 1.0)
    times = {"wq": 1.0, "wk": 1.0, "wv": 2.0, "wo": layers, "w_gate": 1.0, "w_up": bump(kh, FF, 4.0), "w_down": layers}
    x = together(ka, jax.random.normal(kx, shape, jnp.float32), much_x) * bump(kf, D, 4.0)
    dy = together(kb, jax.random.normal(kdy, shape, jnp.float32), much_dy)
    drawn = {"x": x.astype(jnp.bfloat16), "dy": (loud * dy * (SEQUENCES * TOKENS) ** -0.5).astype(jnp.bfloat16)}
    for key, name in zip(kw, NAMES, strict=True):
        drawn[name] = (jax.random.normal(key, SHAPES[name], jnp.float32) * SHAPES[name][1] ** -0.5 * times[name]).astype(jnp.bfloat16)
    return drawn


def matmul(a, w):
    return jnp.dot(a, w, preferred_element_type=jnp.float32).astype(jnp.bfloat16)


def normed(h):
    wide = h.astype(jnp.float32)
    scale = lax.rsqrt(jnp.mean(wide**2, -1, keepdims=True) + 1e-6)
    return (wide * scale).astype(jnp.bfloat16)


def turned(t, theta):
    half = t.shape[-1] // 2
    angle = jnp.arange(t.shape[0], dtype=jnp.float32)[:, None] * theta ** (-jnp.arange(half, dtype=jnp.float32) / half)
    cos, sin = jnp.cos(angle)[:, None], jnp.sin(angle)[:, None]
    a, b = t[..., :half].astype(jnp.float32), t[..., half:].astype(jnp.float32)
    return jnp.concatenate([a * cos - b * sin, b * cos + a * sin], -1).astype(jnp.bfloat16)


def seen_by(q, k, v):
    tokens, kv = q.shape[0], k.shape[1]
    q = q.reshape(tokens, kv, -1, q.shape[-1])
    scores = jnp.einsum("tgsd,ugd->gstu", q.astype(jnp.float32), k.astype(jnp.float32)) * q.shape[-1] ** -0.5
    place = jnp.arange(tokens)
    weights = jax.nn.softmax(jnp.where(place[:, None] >= place, scores, -jnp.inf), -1).astype(jnp.bfloat16)
    return jnp.einsum("gstu,ugd->tgsd", weights.astype(jnp.float32), v.astype(jnp.float32)).astype(jnp.bfloat16).reshape(tokens, -1)


def layer(h, w):
    a = normed(h)
    q, k = (turned(matmul(a, w[name]).reshape(h.shape[0], -1, HEAD), THETA) for name in ("wq", "wk"))
    h = h + matmul(seen_by(q, k, matmul(a, w["wv"]).reshape(h.shape[0], -1, HEAD)), w["wo"])
    b = normed(h)
    gate = jnp.dot(b, w["w_gate"], preferred_element_type=jnp.float32)
    up = jnp.dot(b, w["w_up"], preferred_element_type=jnp.float32)
    return h + matmul((jax.nn.silu(gate) * up).astype(jnp.bfloat16), w["w_down"])


def stack(weights, h):
    return lax.scan(lambda h, w: (layer(h, w), None), h, weights)[0]


def reference(x, dy, wq, wk, wv, wo, w_gate, w_up, w_down):
    weights = dict(zip(NAMES, (wq, wk, wv, wo, w_gate, w_up, w_down), strict=True))

    def take(so_far, sequence):
        h, by_y = sequence
        _, back = jax.vjp(stack, weights, h)
        by_weights, by_h = back(by_y)
        return jax.tree.map(lambda total, term: total + term.astype(jnp.float32), so_far, by_weights), by_h

    none_yet = {name: jnp.zeros(w.shape, jnp.float32) for name, w in weights.items()}
    by_weights, by_x = lax.scan(take, none_yet, (x, dy))
    return (by_x, *(by_weights[name].astype(jnp.bfloat16) for name in NAMES))
```

```python
import functools
import math

import jax
import jax.numpy as jnp
from jax import lax
from jax.experimental import pallas as pl
from jax.experimental.pallas import tpu as pltpu
from jax.sharding import PartitionSpec as P

bf=jnp.bfloat16; f32=jnp.float32
HEAD=128; THETA=10000; EPS=1e-6
ANY=pl.BlockSpec(memory_space=pl.ANY)
def nn(a,b): return lax.dot_general(a,b,(((1,),(0,)),((),())),preferred_element_type=f32)
def nt(a,b): return lax.dot_general(a,b,(((1,),(1,)),((),())),preferred_element_type=f32)
def tn(a,b): return lax.dot_general(a,b,(((0,),(0,)),((),())),preferred_element_type=f32)
def params(**k): return pltpu.CompilerParams(vmem_limit_bytes=62*2**20,**k)
def tok(b,c): return pl.BlockSpec((b,c),lambda i:(i,0))
def rms(h):
    w=h.astype(f32)
    s=lax.rsqrt(jnp.mean(w*w,-1,keepdims=True)+EPS)
    return w,s
def rms_bwd(w,s,g):
    return g*s-w*(s*s*s*jnp.mean(g*w,-1,keepdims=True))
def turn(t,c,s): return t*c+pltpu.roll(t,HEAD//2,1)*s
class Loads:
    def __init__(self,sem): self.sem=sem; self.c=[]
    def add(self,src,dst):
        self.c.append(pltpu.make_async_copy(src,dst,self.sem.at[len(self.c)]))
        return len(self.c)-1
    def start(self):
        @pl.when(pl.program_id(0)==0)
        def _():
            for c in self.c: c.start()
    def need(self,*ns):
        @pl.when(pl.program_id(0)==0)
        def _():
            for n in ns: self.c[n].wait()
def qkv_store(h,wqkv,c_ref,s_ref,q_ref,k_ref,v_ref):
    w,s=rms(h)
    a=(w*s).astype(bf)
    t=nn(a,wqkv).astype(bf)
    c,sn=c_ref[...],s_ref[...]
    nq=q_ref.shape[1]
    for n in range(0,nq+HEAD,HEAD):
        r=turn(t[:,n:n+HEAD].astype(f32),c,sn).astype(bf)
        if n<nq: q_ref[:,n:n+HEAD]=r
        else: k_ref[...]=r
    v_ref[...]=t[:,nq+HEAD:]
def qkv_fwd(x,wq,wk,wv,c,s,B=512):
    T,D=x.shape; Q=wq.shape[1]
    def body(x_ref,wq_,wk_,wv_,c_ref,s_ref,q_ref,k_ref,v_ref,wqkv,sem):
        L=Loads(sem)
        L.add(wq_,wqkv.at[:,0:Q]); L.add(wk_,wqkv.at[:,Q:Q+HEAD]); L.add(wv_,wqkv.at[:,Q+HEAD:])
        L.start(); L.need(0,1,2)
        qkv_store(x_ref[...],wqkv[...],c_ref,s_ref,q_ref,k_ref,v_ref)
    return pl.pallas_call(body,grid=(T//B,),in_specs=[tok(B,D),ANY,ANY,ANY,tok(B,HEAD),tok(B,HEAD)],
        out_specs=[tok(B,Q),tok(B,HEAD),tok(B,HEAD)],out_shape=[jax.ShapeDtypeStruct((T,n),bf) for n in (Q,HEAD,HEAD)],
        scratch_shapes=[pltpu.VMEM((D,Q+2*HEAD),bf),pltpu.SemaphoreType.DMA((3,))],compiler_params=params())(x,wq,wk,wv,c,s)
def mlp_fwd_qkv(h,o,wo,wg,wu,wd,wq,wk,wv,c,s,B=512):
    T,D=h.shape; Q=wq.shape[1]; F=wg.shape[1]
    def body(h_ref,o_ref,wo_,wg_,wu_,wd_,wq_,wk_,wv_,c_ref,s_ref,h2_ref,h3_ref,q_ref,k_ref,v_ref,wo_s,wg_s,wu_s,wd_s,wqkv,sem):
        L=Loads(sem)
        for a,b in ((wo_,wo_s),(wg_,wg_s),(wu_,wu_s),(wd_,wd_s),(wq_,wqkv.at[:,0:Q]),(wk_,wqkv.at[:,Q:Q+HEAD]),(wv_,wqkv.at[:,Q+HEAD:])): L.add(a,b)
        L.start()
        L.need(0)
        h2=h_ref[...]+nn(o_ref[...],wo_s[...]).astype(bf)
        h2_ref[...]=h2
        w,sc=rms(h2); b=(w*sc).astype(bf)
        L.need(1,2)
        g=nn(b,wg_s[...]); u=nn(b,wu_s[...])
        act=(g*(1/(1+jnp.exp(-g)))*u).astype(bf)
        L.need(3)
        h3=h2+nn(act,wd_s[...]).astype(bf)
        h3_ref[...]=h3
        L.need(4,5,6)
        qkv_store(h3,wqkv[...],c_ref,s_ref,q_ref,k_ref,v_ref)
    return pl.pallas_call(body,grid=(T//B,),in_specs=[tok(B,D),tok(B,Q)]+[ANY]*7+[tok(B,HEAD)]*2,
        out_specs=[tok(B,D),tok(B,D),tok(B,Q),tok(B,HEAD),tok(B,HEAD)],out_shape=[jax.ShapeDtypeStruct((T,n),bf) for n in (D,D,Q,HEAD,HEAD)],
        scratch_shapes=[pltpu.VMEM((Q,D),bf),pltpu.VMEM((D,F),bf),pltpu.VMEM((D,F),bf),pltpu.VMEM((F,D),bf),pltpu.VMEM((D,Q+2*HEAD),bf),pltpu.SemaphoreType.DMA((7,))],
        compiler_params=params())(h,o,wo,wg,wu,wd,wq,wk,wv,c,s)
def mlp_bwd(h,o,dy,wo,wg,wu,wd,first,B=512):
    T,D=h.shape; Q=o.shape[1]; F=wg.shape[1]; H=Q//HEAD
    def body(h_ref,o_ref,dy_ref,wo_,wg_,wu_,wd_,dh_ref,do_ref,dl_ref,go_,gg_,gu_,gd_,wo_s,wg_s,wu_s,wd_s,go,gg,gu,gd,sem):
        i=pl.program_id(0); last=pl.num_programs(0)-1
        L=Loads(sem)
        for a,b in ((wo_,wo_s),(wg_,wg_s),(wu_,wu_s),(wd_,wd_s)): L.add(a,b)
        L.start()
        @pl.when(i==0)
        def _():
            for r in (go,gg,gu,gd): r[...]=jnp.zeros(r.shape,f32)
        dy=dy_ref[...]; o=o_ref[...]
        if first:
            L.need(0)
            h2=h_ref[...]+nn(o,wo_s[...]).astype(bf)
        else: h2=h_ref[...]
        w,sc=rms(h2); b=(w*sc).astype(bf)
        L.need(1,2,3)
        g=nn(b,wg_s[...]); u=nn(b,wu_s[...])
        da=nt(dy,wd_s[...]).astype(bf).astype(f32)
        sg=1/(1+jnp.exp(-g)); sl=g*sg
        act=(sl*u).astype(bf)
        gd[...]+=tn(act,dy)
        dg=(da*u*(sg*(1+g*(1-sg)))).astype(bf)
        du=(da*sl).astype(bf)
        gg[...]+=tn(b,dg)
        gu[...]+=tn(b,du)
        db=nt(dg,wg_s[...])+nt(du,wu_s[...])
        dh=dy+rms_bwd(w,sc,db).astype(bf)
        dh_ref[...]=dh
        if not first: L.need(0)
        go[...]+=tn(o,dh)
        do=nt(dh,wo_s[...]).astype(bf)
        do_ref[...]=do
        e=(lax.broadcasted_iota(jnp.int32,(16,Q),0)==lax.broadcasted_iota(jnp.int32,(16,Q),1)//HEAD).astype(bf)
        x=do.astype(f32)*o.astype(f32)
        hi=x.astype(bf); lo=(x-hi.astype(f32)).astype(bf)
        dl_ref[...]=(nt(e,hi)+nt(e,lo))[:H]
        @pl.when(i==last)
        def _():
            cs=[]
            for n,(acc,buf,out) in enumerate(((gd,wd_s,gd_),(gg,wg_s,gg_),(gu,wu_s,gu_),(go,wo_s,go_))):
                buf[...]=acc[...].astype(bf)
                c=pltpu.make_async_copy(buf,out,sem.at[n]); c.start(); cs.append(c)
            for c in cs: c.wait()
    sh=lambda *s: jax.ShapeDtypeStruct(s,bf)
    return pl.pallas_call(body,grid=(T//B,),in_specs=[tok(B,D),tok(B,Q),tok(B,D)]+[ANY]*4,
        out_specs=[tok(B,D),tok(B,Q),pl.BlockSpec((H,B),lambda i:(0,i))]+[ANY]*4,
        out_shape=[sh(T,D),sh(T,Q),jax.ShapeDtypeStruct((H,T),f32),sh(Q,D),sh(D,F),sh(D,F),sh(F,D)],
        scratch_shapes=[pltpu.VMEM(s,bf) for s in ((Q,D),(D,F),(D,F),(F,D))]+[pltpu.VMEM(s,f32) for s in ((Q,D),(D,F),(D,F),(F,D))]+[pltpu.SemaphoreType.DMA((4,))],
        compiler_params=params())(h,o,dy,wo,wg,wu,wd)
def qkv_bwd(h,dh,dq,dk,dv,wq,wk,wv,c,s,B=512):
    T,D=h.shape; Q=wq.shape[1]
    def body(h_ref,dh_ref,dq_ref,dk_ref,dv_ref,wq_,wk_,wv_,c_ref,s_ref,dx_ref,gq_,gk_,gv_,wqkv,gacc,t_s,sem):
        i=pl.program_id(0); last=pl.num_programs(0)-1
        L=Loads(sem)
        L.add(wq_,wqkv.at[:,0:Q]); L.add(wk_,wqkv.at[:,Q:Q+HEAD]); L.add(wv_,wqkv.at[:,Q+HEAD:])
        L.start()
        @pl.when(i==0)
        def _(): gacc[...]=jnp.zeros(gacc.shape,f32)
        cs,sn=c_ref[...],-s_ref[...]
        for n in range(0,Q,HEAD): t_s[:,n:n+HEAD]=turn(dq_ref[:,n:n+HEAD].astype(f32),cs,sn).astype(bf)
        t_s[:,Q:Q+HEAD]=turn(dk_ref[...].astype(f32),cs,sn).astype(bf)
        t_s[:,Q+HEAD:]=dv_ref[...]
        t=t_s[...]
        w,sc=rms(h_ref[...]); a=(w*sc).astype(bf)
        gacc[...]+=tn(a,t)
        L.need(0,1,2)
        da=nt(t,wqkv[...])
        dx_ref[...]=dh_ref[...]+rms_bwd(w,sc,da).astype(bf)
        @pl.when(i==last)
        def _():
            wqkv[...]=gacc[...].astype(bf)
            cc=[pltpu.make_async_copy(wqkv.at[:,0:Q],gq_,sem.at[0]),pltpu.make_async_copy(wqkv.at[:,Q:Q+HEAD],gk_,sem.at[1]),pltpu.make_async_copy(wqkv.at[:,Q+HEAD:],gv_,sem.at[2])]
            for x in cc: x.start()
            for x in cc: x.wait()
    sh=lambda *s: jax.ShapeDtypeStruct(s,bf)
    return pl.pallas_call(body,grid=(T//B,),in_specs=[tok(B,D),tok(B,D),tok(B,Q),tok(B,HEAD),tok(B,HEAD)]+[ANY]*3+[tok(B,HEAD)]*2,
        out_specs=[tok(B,D)]+[ANY]*3,out_shape=[sh(T,D),sh(D,Q),sh(D,HEAD),sh(D,HEAD)],
        scratch_shapes=[pltpu.VMEM((D,Q+2*HEAD),bf),pltpu.VMEM((D,Q+2*HEAD),f32),pltpu.VMEM((B,Q+2*HEAD),bf),pltpu.SemaphoreType.DMA((3,))],
        compiler_params=params())(h,dh,dq,dk,dv,wq,wk,wv,c,s)
def tables(T):
    half=HEAD//2
    ang=jnp.arange(T,dtype=f32)[:,None]*THETA**(-jnp.arange(half,dtype=f32)/half)
    c,s=jnp.cos(ang),jnp.sin(ang)
    return jnp.concatenate([c,c],-1),jnp.concatenate([-s,s],-1)
MESH=pl.DeviceIdType.MESH
def place(side):
    me=lax.axis_index("dp"); rep=lax.axis_index("rep")
    return lax.div(me,side),lax.rem(me,side),rep,lax.rem(rep,2)
def greet(side,partner):
    x,y,rep,core=place(side)
    bar=pltpu.get_barrier_semaphore()
    n=0
    for k in range(1,side):
        for t in (lax.rem(x+k,side)*side+y, x*side+lax.rem(y+k,side)):
            pl.semaphore_signal(bar,inc=1,device_id={"dp":t},device_id_type=MESH); n+=1
    if partner:
        pl.semaphore_signal(bar,inc=1,device_id={"rep":rep+1-2*core},device_id_type=MESH); n+=1
    pl.semaphore_wait(bar,n)
class Gather:
    def __init__(self,side,pieces,sems):
        self.side=side; self.n=len(pieces)
        x,y,rep,core=place(side)
        self.local,self.send0,self.recv0,self.send1,self.recv1,self.hand,self.take=[],[],[],[],[],[],[]
        s0,r0,s1,r1,sh,rh,lo=sems
        me_side=range(1,side)
        for p,(src,dst,xf,sl) in enumerate(pieces):
            mine=(slice(None),slice(None)) if sl is None else sl(core)
            other=None if sl is None else sl(1-core)
            own=dst.at[(x,y)+mine]
            self.local.append(pltpu.make_async_copy(src.at[mine],own,lo.at[p]))
            dev=lambda k,first: {"dp":(lax.rem(x+k,side)*side+y) if (xf==first) else (x*side+lax.rem(y+k,side))}
            slot=lambda d: (lax.rem(x+side-d,side),y) if xf else (x,lax.rem(y+side-d,side))
            line=lambda d,sl_: dst.at[((slice(None),lax.rem(y+side-d,side)) if xf else (lax.rem(x+side-d,side),slice(None)))+sl_]
            mk=lambda a,b,s,r,to: pltpu.make_async_remote_copy(a,b,s,r,device_id=to,device_id_type=MESH)
            self.send0.append([mk(src.at[mine],own,s0.at[p,k-1],r0.at[p,k-1],dev(k,True)) for k in me_side])
            self.recv0.append([mk(src.at[mine],dst.at[slot(k)+mine],s0.at[p,k-1],r0.at[p,k-1],dev(k,True)) for k in me_side])
            self.send1.append([mk(line(0,mine),line(0,mine),s1.at[p,k-1],r1.at[p,k-1],dev(k,False)) for k in me_side])
            self.recv1.append([mk(line(k,mine),line(k,mine),s1.at[p,k-1],r1.at[p,k-1],dev(k,False)) for k in me_side])
            if sl is None: self.hand.append([]); self.take.append([])
            else:
                to={"rep":rep+1-2*core}
                self.hand.append([mk(line(k,mine),line(k,mine),sh.at[p,k],rh.at[p,k],to) for k in range(side)])
                self.take.append([mk(line(k,other),line(k,other),sh.at[p,k],rh.at[p,k],to) for k in range(side)])
    @staticmethod
    def scratch(n,side):
        D=pltpu.SemaphoreType.DMA
        return [D((n,side-1))]*4+[D((n,side))]*2+[D((n,))]
    def start(self):
        greet(self.side,any(self.hand))
        for c in self.local: c.start()
        for p in range(self.n):
            for c in self.send0[p]: c.start()
    def mid(self,ps):
        for p in ps:
            self.local[p].wait()
            for c in self.recv0[p]: c.wait_recv()
            for c in self.send1[p]: c.start()
            for c in self.hand[p][:1]: c.start()
    def late(self,ps):
        for p in ps:
            for k,c in enumerate(self.recv1[p]):
                c.wait_recv()
                if self.hand[p]: self.hand[p][k+1].start()
    def finish(self):
        for p in range(self.n):
            for c in self.take[p]: c.wait_recv()
            for c in self.send0[p]+self.send1[p]+self.hand[p]: c.wait_send()
class Scatter:
    def __init__(self,side,pieces,bufs,sems):
        self.side=side; self.n=len(pieces)
        x,y,rep,core=place(side)
        self.load,self.send0,self.recv0,self.send1,self.recv1,self.store=[],[],[],[],[],[]
        self.bufs=[]; self.at=[]
        s0,r0,s1,r1,lo,st=sems
        for p,(src,out,xf,sl) in enumerate(pieces):
            own,got0,half,got1,done=bufs[p*5:p*5+5]
            self.bufs.append((own,got0,half,got1,done)); self.at.append(y if xf else x)
            line=lambda d: src.at[((lax.rem(x+d,side),slice(None)) if xf else (slice(None),lax.rem(y+d,side)))+sl]
            dev=lambda k,first: {"dp":(lax.rem(x+k,side)*side+y) if (xf==first) else (x*side+lax.rem(y+k,side))}
            mk=lambda a,b,s,r,to: pltpu.make_async_remote_copy(a,b,s,r,device_id=to,device_id_type=MESH)
            self.load.append(pltpu.make_async_copy(line(0),own,lo.at[p]))
            self.send0.append([mk(line(k),got0.at[k-1],s0.at[p,k-1],r0.at[p,k-1],dev(k,True)) for k in range(1,side)])
            self.send1.append([mk(half.at[lax.rem((y if xf else x)+k,side)],got1.at[k-1],s1.at[p,k-1],r1.at[p,k-1],dev(k,False)) for k in range(1,side)])
            self.store.append(pltpu.make_async_copy(done,out.at[sl],st.at[p]))
    @staticmethod
    def scratch(shapes,side):
        b=[]
        for r,c in shapes:
            b+=[pltpu.VMEM((side,r,c),bf),pltpu.VMEM((side-1,side,r,c),bf),pltpu.VMEM((side,r,c),bf),pltpu.VMEM((side-1,r,c),bf),pltpu.VMEM((r,c),bf)]
        D=pltpu.SemaphoreType.DMA; n=len(shapes)
        return b,[D((n,side-1))]*4+[D((n,))]*2
    def start(self):
        greet(self.side,False)
        self.begin()
    def begin(self):
        for p in range(self.n):
            for c in self.send0[p]: c.start()
            self.load[p].start()
    def mid(self,ps):
        for p in ps:
            own,got0,half,_,_=self.bufs[p]
            self.load[p].wait()
            for c in self.send0[p]: c.wait_recv()
            def one(t,_,own=own,got0=got0,half=half):
                a=own[t].astype(f32)
                for k in range(self.side-1): a=a+got0[k,t].astype(f32)
                half[t]=a.astype(bf)
                return 0
            lax.fori_loop(0,self.side,one,0)
            for c in self.send1[p]: c.start()
    def late(self,ps):
        for p in ps:
            own,got0,half,got1,done=self.bufs[p]; t=self.at[p]
            for c in self.send1[p]: c.wait_recv()
            a=own[t].astype(f32)
            for k in range(self.side-1): a=a+got0[k,t].astype(f32)
            for k in range(self.side-1): a=a+got1[k].astype(f32)
            done[...]=a.astype(bf)
            self.store[p].start()
    def finish(self):
        for p in range(self.n):
            for c in self.send0[p]+self.send1[p]: c.wait_send()
            self.store[p].wait()
NEG=-1e30; HIDDEN=-2e30; LOG2E=1.4426950408889634
BQ=512; HALF=256
def sd(*s,dt=bf): return jax.ShapeDtypeStruct(s,dt)
def columns(size,n,parts):
    each=size//2//parts
    return lambda core: (slice(None),pl.ds(pl.multiple_of(core*(size//2)+n*each,128),each))
def half_rows(size):
    return lambda core: (pl.ds(pl.multiple_of(core*(size//2),8),size//2),slice(None))
def gather_pieces(srcs,dsts):
    out=[]; flip=[True,True]
    for src,dst in zip(srcs,dsts):
        r,c=src.shape
        if c==HEAD: out.append((src,dst,flip[0],None)); flip[0]=not flip[0]
        elif r%16==0: out.append((src,dst,flip[1],half_rows(r))); flip[1]=not flip[1]
        else: out+=[(src,dst,n==0,columns(c,n,2)) for n in range(2)]
    return out
def count_gather(shapes): return sum(2 if c!=HEAD and r%16 else 1 for r,c in shapes)
def scatter_cuts(shapes):
    out=[]; flip=True
    for n,(r,c) in enumerate(shapes):
        if c==HEAD: out.append((n,flip,(slice(None),slice(None)),(r,c))); flip=not flip
        elif r%16==0: out+=[(n,h==0,(slice(h*(r//2),(h+1)*(r//2)),slice(None)),(r//2,c)) for h in range(2)]
        else: out+=[(n,h==0,(slice(None),slice(h*(c//2),(h+1)*(c//2))),(r,c//2)) for h in range(2)]
    return out
def attend(q,k,v,srcs,layers,side,cid,hooks):
    T,Q=q.shape; d=HEAD; H=Q//d; n_src=len(srcs)
    e=d**-0.5*LOG2E; wide=HALF; cols=H*BQ
    shapes=[s.shape[1:] for s in srcs]; np_=count_gather(shapes)
    def body(q_ref,k_ref,v_ref,*rest):
        src,rest=rest[:n_src],rest[n_src:]
        o_ref,lse_ref=rest[:2]; dst=rest[2:2+n_src]; top_s,mix_s=rest[2+n_src:4+n_src]; sems=rest[4+n_src:]
        i=pl.program_id(0)
        G=Gather(side,gather_pieces([s.at[l] for s,l in zip(src,layers)],dst),sems)
        def fire(j,diag):
            for hi,hj,what,a,b in hooks:
                if diag!=(hj==-1) or hj==-2: continue
                ps=range(a*np_//12,b*np_//12)
                cond=(i==hi) if diag else (i==hi)&(j==hj)
                @pl.when(cond)
                def _(): getattr(G,what)(ps)
        @pl.when(i==0)
        def _(): G.start()
        top_s[...]=jnp.full(top_s.shape,NEG,f32)
        mix_s[...]=jnp.zeros(mix_s.shape,f32)
        def run(pieces,ahead):
            kc={}
            def kv(key0,nk):
                if nk not in kc:
                    here=pl.ds(key0,nk)
                    kc[nk]=(k_ref[here,:],jnp.concatenate([v_ref[here,:].T,jnp.ones((8,nk),bf)],axis=0))
                return kc[nk]
            def scores(p):
                h,q0,key0,nk,off=p
                return nt(kv(key0,nk)[0],q_ref[q0:q0+wide,h*d:(h+1)*d])
            def soft(p,s):
                h,q0,key0,nk,off=p
                c=slice(h*BQ+q0,h*BQ+q0+wide)
                if off is not None:
                    gap=lax.broadcasted_iota(jnp.int32,(nk,wide),1)-lax.broadcasted_iota(jnp.int32,(nk,wide),0)
                    s=jnp.where(gap>=off,s,HIDDEN)
                old=top_s[0:1,c]
                top=jnp.maximum(old,s.max(axis=0,keepdims=True))
                top_s[0:1,c]=top
                return jnp.exp2((s-top)*e).astype(bf),jnp.exp2((old-top)*e)
            def mix(p,w,keep):
                h,q0,key0,nk,off=p
                c=slice(h*BQ+q0,h*BQ+q0+wide)
                mix_s[:,c]=mix_s[:,c]*keep+nn(kv(key0,nk)[1],w)
            n_p=len(pieces); ss={}; ws={}
            for n in range(n_p+2*ahead):
                if n<n_p: ss[n]=scores(pieces[n])
                m=n-ahead
                if 0<=m<n_p: ws[m]=soft(pieces[m],ss.pop(m))
                m=n-2*ahead
                if 0<=m<n_p: mix(pieces[m],*ws.pop(m))
        def whole(j,_):
            fire(j,False)
            key0=pl.multiple_of(j*BQ,BQ)
            run([(h,q0,key0,BQ,None) for h in range(H) for q0 in range(0,BQ,wide)],4)
            return 0
        lax.fori_loop(0,i,whole,0)
        fire(None,True)
        base=pl.multiple_of(i*BQ,BQ)
        run([(h,t*wide,base,(t+1)*wide,-t*wide) for h in range(H) for t in range(BQ//wide)],4)
        for h in range(H):
            c=slice(h*BQ,(h+1)*BQ)
            total=mix_s[d:d+1,c]
            o_ref[:,h*d:(h+1)*d]=(mix_s[:d,c]*(1/total)).T.astype(bf)
            lse_ref[h:h+1,:]=top_s[0:1,c]*(d**-0.5)+jnp.log(total)
        @pl.when(i==pl.num_programs(0)-1)
        def _():
            for hi,hj,what,a,b in hooks:
                if hj==-2: getattr(G,what)(range(a*np_//12,b*np_//12))
            G.finish()
    whole_kv=pl.BlockSpec((T,d),lambda i:(0,0))
    return pl.pallas_call(body,grid=(T//BQ,),in_specs=[tok(BQ,Q),whole_kv,whole_kv]+[ANY]*n_src,
        out_specs=[tok(BQ,Q),pl.BlockSpec((H,BQ),lambda i:(0,i))]+[ANY]*n_src,
        out_shape=[sd(T,Q),sd(H,T,dt=f32)]+[sd(side,side,*s) for s in shapes],
        scratch_shapes=[pltpu.VMEM((1,cols),f32),pltpu.VMEM((d+8,cols),f32)]+Gather.scratch(np_,side),
        compiler_params=params(collective_id=cid,has_side_effects=True))(q,k,v,*srcs)
def attend_bwd(q,k,v,do,lse,delta,grads,side,cid,hooks):
    T,Q=q.shape; d=HEAD; H=Q//d; scale=d**-0.5; e=scale*LOG2E; n_g=len(grads); wide=BQ
    shapes=[g.shape[2:] for g in grads]; cuts=scatter_cuts(shapes); np_=len(cuts)
    bufs,sems=Scatter.scratch([c[3] for c in cuts],side)
    def body(q_ref,k_ref,v_ref,do_ref,lse_ref,delta_ref,*rest):
        g_ref,rest=rest[:n_g],rest[n_g:]
        dq_ref,dk_ref,dv_ref=rest[:3]; out=rest[3:3+n_g]; dq_s,dk_s,dv_s=rest[3+n_g:6+n_g]; rest=rest[6+n_g:]
        i=pl.program_id(0)
        S=Scatter(side,[(g_ref[n],out[n],xf,sl) for n,xf,sl,_ in cuts],rest[:5*np_],rest[5*np_:])
        def fire(j,diag):
            for hi,hj,what,a,b in hooks:
                if diag!=(hj==-1) or hj==-2: continue
                @pl.when((i==hi) if diag else (i==hi)&(j==hj))
                def _(): getattr(S,what)(range(a*np_//12,b*np_//12))
        @pl.when(i==0)
        def _():
            S.start()
            dk_s[...]=jnp.zeros(dk_s.shape,f32); dv_s[...]=jnp.zeros(dv_s.shape,f32)
        dq_s[...]=jnp.zeros(dq_s.shape,f32)
        lse2=lse_ref[...]*LOG2E
        def run(pieces,key0,ahead):
            kc={}; acc={}
            def kv(nk):
                if nk not in kc:
                    here=pl.ds(key0,nk)
                    kc[nk]=(k_ref[here,:],v_ref[here,:],k_ref[here,:].T)
                return kc[nk]
            qs=lambda p: q_ref[p[1]:p[1]+p[2],p[0]*d:(p[0]+1)*d]
            dos=lambda p: do_ref[p[1]:p[1]+p[2],p[0]*d:(p[0]+1)*d]
            def scores(p): return nt(kv(p[3])[0],qs(p)),nt(kv(p[3])[1],dos(p))
            def weigh(p,s,dp):
                h,q0,w,nk,off=p
                x=jnp.exp2(s*e-lse2[h:h+1,q0:q0+w])
                if off is not None:
                    gap=lax.broadcasted_iota(jnp.int32,(nk,w),1)-lax.broadcasted_iota(jnp.int32,(nk,w),0)
                    x=jnp.where(gap>=off,x,0.0)
                return x.astype(bf),(x*(dp-delta_ref[h:h+1,q0:q0+w])).astype(bf)
            def add(p,x,ds):
                h,q0,w,nk,off=p
                a,b=nn(x,dos(p)),nn(ds,qs(p))
                acc[nk]=(acc[nk][0]+a,acc[nk][1]+b) if nk in acc else (a,b)
                c=slice(h*BQ+q0,h*BQ+q0+w)
                dq_s[:,c]+=nn(kv(nk)[2],ds)
            n_p=len(pieces); ss={}; ws={}
            for n in range(n_p+2*ahead):
                if n<n_p: ss[n]=scores(pieces[n])
                m=n-ahead
                if 0<=m<n_p: ws[m]=weigh(pieces[m],*ss.pop(m))
                m=n-2*ahead
                if 0<=m<n_p: add(pieces[m],*ws.pop(m))
            for nk,(a,b) in acc.items():
                here=pl.ds(key0,nk)
                dv_s[here,:]+=a; dk_s[here,:]+=b
        def block(j,_):
            fire(j,False)
            run([(h,0,BQ,BQ,None) for h in range(H)],pl.multiple_of(j*BQ,BQ),2)
            return 0
        lax.fori_loop(0,i,block,0)
        fire(None,True)
        run([(h,t*HALF,HALF,(t+1)*HALF,-t*HALF) for t in range(BQ//HALF) for h in range(H)],pl.multiple_of(i*BQ,BQ),2)
        for h in range(H): dq_ref[:,h*d:(h+1)*d]=(dq_s[:,h*BQ:(h+1)*BQ]*scale).T.astype(bf)
        @pl.when(i==pl.num_programs(0)-1)
        def _():
            dk_ref[...]=(dk_s[...]*scale).astype(bf); dv_ref[...]=dv_s[...].astype(bf)
            for hi,hj,what,a,b in hooks:
                if hj==-2: getattr(S,what)(range(a*np_//12,b*np_//12))
            S.finish()
    whole_kv=pl.BlockSpec((T,d),lambda i:(0,0)); rows=pl.BlockSpec((H,BQ),lambda i:(0,i))
    return pl.pallas_call(body,grid=(T//BQ,),in_specs=[tok(BQ,Q),whole_kv,whole_kv,tok(BQ,Q),rows,rows]+[ANY]*n_g,
        out_specs=[tok(BQ,Q),whole_kv,whole_kv]+[ANY]*n_g,
        out_shape=[sd(T,Q),sd(T,d),sd(T,d)]+[sd(*s) for s in shapes],
        scratch_shapes=[pltpu.VMEM((d,H*BQ),f32),pltpu.VMEM((T,d),f32),pltpu.VMEM((T,d),f32)]+bufs+sems,
        compiler_params=params(collective_id=cid,has_side_effects=True))(q,k,v,do,lse,delta,*grads)
def fetch(srcs,layers,side,cid):
    shapes=[s.shape[1:] for s in srcs]; np_=count_gather(shapes); n=len(srcs)
    def body(*refs):
        G=Gather(side,gather_pieces([s.at[l] for s,l in zip(refs[:n],layers)],refs[n:2*n]),refs[2*n:])
        G.start(); G.mid(range(np_)); G.late(range(np_)); G.finish()
    return pl.pallas_call(body,in_specs=[ANY]*n,out_specs=[ANY]*n,out_shape=[sd(side,side,*s) for s in shapes],
        scratch_shapes=Gather.scratch(np_,side),compiler_params=params(collective_id=cid,has_side_effects=True))(*srcs)
def collect(grads,side,cid):
    shapes=[g.shape[2:] for g in grads]; cuts=scatter_cuts(shapes); np_=len(cuts); n_g=len(grads)
    bufs,sems=Scatter.scratch([c[3] for c in cuts],side)
    def body(*refs):
        rest=refs[2*n_g:]
        S=Scatter(side,[(refs[n],refs[n_g+n],xf,sl) for n,xf,sl,_ in cuts],rest[:5*np_],rest[5*np_:])
        S.start(); S.mid(range(np_)); S.late(range(np_)); S.finish()
    return pl.pallas_call(body,in_specs=[ANY]*n_g,out_specs=[ANY]*n_g,out_shape=[sd(*s) for s in shapes],
        scratch_shapes=bufs+sems,compiler_params=params(collective_id=cid,has_side_effects=True))(*grads)
FETCH=((1,-1,"mid",0,12),(3,0,"late",0,4),(3,1,"late",4,7),(3,2,"late",7,9),(3,-1,"late",9,11),(3,-2,"late",11,12))
SUM=((3,1,"mid",0,6),(3,2,"mid",6,12),(3,-2,"late",0,12))
def solution(mesh):
    side=math.isqrt(mesh.shape["dp"])
    def step(x,dy,wq,wk,wv,wo,wg,wu,wd):
        x,dy=x[0],dy[0]
        c,s=tables(x.shape[0])
        flat=lambda ws: [w.reshape(-1,w.shape[-1]) for w in ws]
        cut=lambda gs: [g.reshape(side,side,-1,g.shape[-1]) for g in gs]
        qkv0=flat(fetch((wq,wk,wv),(0,0,0),side,0))
        q0,k0,v0=qkv_fwd(x,*qkv0,c,s)
        o0,l0,*w=attend(q0,k0,v0,(wo,wg,wu,wd,wq,wk,wv),(0,0,0,0,1,1,1),side,1,FETCH)
        w=flat(w); mlp0,qkv1=w[:4],w[4:]
        h2,h3,q1,k1,v1=mlp_fwd_qkv(x,o0,*mlp0,*qkv1,c,s)
        o1,l1,*w=attend(q1,k1,v1,(wo,wg,wu,wd),(1,1,1,1),side,2,FETCH)
        mlp1=flat(w)
        dh,do,dl,*gm1=mlp_bwd(h3,o1,dy,*mlp1,True)
        dq,dk,dv,*sm1=attend_bwd(q1,k1,v1,do,l1,dl,cut(gm1),side,3,SUM)
        dx,*gq1=qkv_bwd(h3,dh,dq,dk,dv,*qkv1,c,s)
        dh,do,dl,*gm0=mlp_bwd(h2,o0,dx,*mlp0,False)
        dq,dk,dv,*sums=attend_bwd(q0,k0,v0,do,l0,dl,cut(gm0+gq1),side,4,SUM)
        sm0,sq1=sums[:4],sums[4:]
        dx,*gq0=qkv_bwd(x,dh,dq,dk,dv,*qkv0,c,s)
        sq0=collect(cut(gq0),side,5)
        return (dx[None],*(jnp.stack(p) for p in zip(list(sq0)+list(sm0),list(sq1)+list(sm1))))
    states,cut_=P(("rep","dp"),None,None),P(None,"dp",None)
    return jax.shard_map(step,mesh=mesh,in_specs=(states,states)+(cut_,)*7,out_specs=(states,)+(P("rep","dp",None),)*7,check_vma=False)
```
